32 devices in a mesh: dp: 16 (over z, x, core), tensor: 2 (over y).
Axes of the slice: x: 2, y: 2, z: 4, core: 2. Of those that a mesh axis runs over, the one named last changes fastest.
Arguments:
- inputs: bfloat16 [16, 256, 4096], P('dp', 'tensor'), may hold values from -40 to 40
- query_states: bfloat16 [16, 256, 3072], P('dp', None, 'tensor'), may hold values from -4.5 to 4.5
- key_states: bfloat16 [16, 256, 1024], P('dp', None, 'tensor'), may hold values from -4.5 to 4.5
- saved_value_states: bfloat16 [16, 256, 1024], P('dp', None, 'tensor'), may hold values from -4.5 to 4.5
- head_cotangent: bfloat16 [16, 256, 3072], P('dp', None, 'tensor'), may hold values from -40 to 40
- query_weight: bfloat16 [4096, 3072], P('dp', 'tensor'), may hold values from -0.09375 to 0.09375
- key_matrix: bfloat16 [4096, 1024], P('dp', 'tensor'), may hold values from -0.09375 to 0.09375
- value_matrix: bfloat16 [4096, 1024], P('dp', 'tensor'), may hold values from -0.09375 to 0.09375
- query_momentum: float32 [4096, 3072], P('dp', 'tensor'), may hold values from -6 to 6
- key_prior_momentum: float32 [4096, 1024], P('dp', 'tensor'), may hold values from -6 to 6
- value_prior_momentum: float32 [4096, 1024], P('dp', 'tensor'), may hold values from -6 to 6
Outputs:
- input_gradient: bfloat16 [16, 256, 4096], P('dp', 'tensor')
- query_velocity: float32 [4096, 3072], P('dp', 'tensor')
- key_velocity: float32 [4096, 1024], P('dp', 'tensor')
- value_velocity: float32 [4096, 1024], P('dp', 'tensor')
The draws below stay inside these ranges and needn't reach their ends.
All inputs are finite; a program needn't handle non-finite values.
Results may differ from the reference program's by a relative error of at most 0.019.
Values may be sent and summed in bfloat16 or wider, within the bound.
A program may use at most 128 MiB of HBM per device.

```python
import math
import jax
import jax.numpy as jnp
from jax import lax

MODEL_FEATURES = 4096
QUERY_HEADS = 24
KEY_VALUE_HEADS = 8
HEAD_SIZE = 128
SEQUENCE_LENGTH = 256
SEQUENCE_COUNT = 16
N_TENSOR = 2


def column_scales(base_key, width, head_width):
    spread = jnp.exp(jax.random.uniform(base_key, (width,), jnp.float32, math.log(0.3), math.log(3.0)))
    position = (jnp.arange(width, dtype=jnp.int32) // head_width).astype(jnp.float32)
    last_index = max(width // head_width - 1, 1)
    rising = jnp.exp(math.log(3.0) * (position / last_index - 0.5))
    return (spread, rising)


def draw_scaled(base_key, array_shape, head_width):
    key_scale, key_noise = jax.random.split(base_key, 2)
    width = array_shape[-1]
    spread, rising = column_scales(key_scale, width, head_width)
    value_entries = jnp.clip(jax.random.normal(key_noise, array_shape, jnp.float32), -4.0, 4.0) * spread * rising
    return value_entries


def draw_inputs(key, part):
    return draw_scaled(jax.random.fold_in(key, 11), (SEQUENCE_COUNT, SEQUENCE_LENGTH, MODEL_FEATURES), 1).astype(jnp.bfloat16)


def draw_head_cotangent(key, part):
    return draw_scaled(jax.random.fold_in(key, 13), (SEQUENCE_COUNT, SEQUENCE_LENGTH, QUERY_HEADS * HEAD_SIZE), HEAD_SIZE).astype(jnp.bfloat16)


def draw_query_states(key, part):
    base_key = jax.random.fold_in(key, 17)
    array_shape = (SEQUENCE_COUNT, SEQUENCE_LENGTH, QUERY_HEADS, HEAD_SIZE)
    value_entries = jnp.clip(jax.random.normal(base_key, array_shape, jnp.float32), -4.5, 4.5)
    return value_entries.reshape(SEQUENCE_COUNT, SEQUENCE_LENGTH, QUERY_HEADS * HEAD_SIZE).astype(jnp.bfloat16)


def draw_key_states(key, part):
    base_key = jax.random.fold_in(key, 19)
    array_shape = (SEQUENCE_COUNT, SEQUENCE_LENGTH, KEY_VALUE_HEADS, HEAD_SIZE)
    value_entries = jnp.clip(jax.random.normal(base_key, array_shape, jnp.float32), -4.5, 4.5)
    return value_entries.reshape(SEQUENCE_COUNT, SEQUENCE_LENGTH, KEY_VALUE_HEADS * HEAD_SIZE).astype(jnp.bfloat16)


def block_levels(own_key, extent, cuts, low, top_value):
    gain, own = 1.0, jax.random.fold_in(own_key, 6)
    for dim, shards_of in cuts:
        draws = jnp.exp(jax.random.uniform(jax.random.fold_in(own, dim), (shards_of,), jnp.float32, low / len(cuts), top_value / len(cuts)))
        gain = gain * jnp.repeat(draws, extent[dim] // shards_of).reshape([-1 if axis == dim else 1 for axis in range(len(extent))])
    return gain


def scatter_about(rng, extent, deviation, limit, shards=(), kind=jnp.bfloat16):
    values = deviation * jax.random.normal(rng, extent, jnp.float32)
    if shards:
        values = values * block_levels(rng, extent, shards, -0.22, 0.18)
    return jnp.clip(values, -limit, limit).astype(kind)


def setup_inputs(seed: int = 0) -> dict:
    arg_keys = jax.random.split(jax.random.key(seed), 12)
    return {
        "inputs": draw_inputs(jax.random.fold_in(arg_keys[11], 71), 0),
        "query_states": draw_query_states(jax.random.fold_in(arg_keys[11], 71), 0),
        "key_states": draw_key_states(jax.random.fold_in(arg_keys[11], 71), 0),
        "saved_value_states": scatter_about(arg_keys[3], (SEQUENCE_COUNT, SEQUENCE_LENGTH, KEY_VALUE_HEADS * HEAD_SIZE), 1.0, 4.5, ((0, 16), (2, 2))),
        "head_cotangent": draw_head_cotangent(jax.random.fold_in(arg_keys[11], 71), 0),
        "query_weight": scatter_about(arg_keys[5], (MODEL_FEATURES, QUERY_HEADS * HEAD_SIZE), MODEL_FEATURES ** -0.5, 0.09375, ((0, 16), (1, 2))),
        "key_matrix": scatter_about(arg_keys[6], (MODEL_FEATURES, KEY_VALUE_HEADS * HEAD_SIZE), MODEL_FEATURES ** -0.5, 0.09375, ((0, 16), (1, 2))),
        "value_matrix": scatter_about(arg_keys[7], (MODEL_FEATURES, KEY_VALUE_HEADS * HEAD_SIZE), MODEL_FEATURES ** -0.5, 0.09375, ((0, 16), (1, 2))),
        "query_momentum": scatter_about(arg_keys[8], (MODEL_FEATURES, QUERY_HEADS * HEAD_SIZE), 1.0, 6.0, ((0, 16), (1, 2)), jnp.float32),
        "key_prior_momentum": scatter_about(arg_keys[9], (MODEL_FEATURES, KEY_VALUE_HEADS * HEAD_SIZE), 1.0, 6.0, ((0, 16), (1, 2)), jnp.float32),
        "value_prior_momentum": scatter_about(arg_keys[10], (MODEL_FEATURES, KEY_VALUE_HEADS * HEAD_SIZE), 1.0, 6.0, ((0, 16), (1, 2)), jnp.float32),
    }


def rounded(value_entries):
    return lax.optimization_barrier(value_entries.astype(jnp.bfloat16)).astype(jnp.float32)

def sequence_backward(sequence_queries, sequence_keys, sequence_values, sequence_cotangent):
    token_length = sequence_queries.shape[0]
    group_width = QUERY_HEADS // KEY_VALUE_HEADS
    scaling = 1.0 / math.sqrt(HEAD_SIZE)
    query_quad = sequence_queries.astype(jnp.float32).reshape(token_length, KEY_VALUE_HEADS, group_width, HEAD_SIZE)
    cotangent_quad = sequence_cotangent.astype(jnp.float32).reshape(token_length, KEY_VALUE_HEADS, group_width, HEAD_SIZE)
    key_triple = sequence_keys.astype(jnp.float32).reshape(token_length, KEY_VALUE_HEADS, HEAD_SIZE)
    value_triple = sequence_values.astype(jnp.float32).reshape(token_length, KEY_VALUE_HEADS, HEAD_SIZE)
    scores = jnp.einsum('ihgd,jhd->hgij', query_quad, key_triple) * scaling
    position = jnp.arange(token_length, dtype=jnp.int32)
    causal = position[:, None] >= position[None, :]
    scores = jnp.where(causal, scores, -jnp.inf)
    maximum = lax.optimization_barrier(jnp.max(scores, axis=-1, keepdims=True))
    exponent = jnp.exp(scores - maximum)
    softmax_rows = exponent / lax.optimization_barrier(jnp.sum(exponent, axis=-1, keepdims=True))
    softmax_reduced = rounded(softmax_rows)
    grad_softmax = jnp.einsum('ihgd,jhd->hgij', cotangent_quad, value_triple)
    row_delta = lax.optimization_barrier(jnp.sum(softmax_rows * grad_softmax, axis=-1, keepdims=True))
    score_gradient = rounded(softmax_rows * (grad_softmax - row_delta) * scaling)
    grad_query = jnp.einsum('hgij,jhd->ihgd', score_gradient, key_triple).astype(jnp.bfloat16).reshape(token_length, QUERY_HEADS * HEAD_SIZE)
    key_gradient = jnp.einsum('xfwo,wxfp->oxp', score_gradient, query_quad).astype(jnp.bfloat16).reshape(token_length, KEY_VALUE_HEADS * HEAD_SIZE)
    value_gradient = jnp.einsum('xfwo,wxfp->oxp', softmax_reduced, cotangent_quad).astype(jnp.bfloat16).reshape(token_length, KEY_VALUE_HEADS * HEAD_SIZE)
    return (grad_query, key_gradient, value_gradient)

def reference(inputs, query_states, key_states, saved_value_states, head_cotangent, query_weight, key_matrix, value_matrix, query_momentum, key_prior_momentum, value_prior_momentum):
    query_share = QUERY_HEADS * HEAD_SIZE // N_TENSOR
    paired_portion = KEY_VALUE_HEADS * HEAD_SIZE // N_TENSOR

    def one_sequence(running, sequence_slices):
        input_seq, sequence_queries, sequence_keys, sequence_values, sequence_cotangent = sequence_slices
        grad_query, key_gradient, value_gradient = sequence_backward(sequence_queries, sequence_keys, sequence_values, sequence_cotangent)
        summed = jnp.zeros((input_seq.shape[0], MODEL_FEATURES), jnp.float32)
        for block_index in range(N_TENSOR):
            query_span = slice(block_index * query_share, (block_index + 1) * query_share)
            pair_span = slice(block_index * paired_portion, (block_index + 1) * paired_portion)
            partial_value = jnp.dot(grad_query[:, query_span], query_weight[:, query_span].T, preferred_element_type=jnp.float32)
            partial_value = partial_value + jnp.dot(key_gradient[:, pair_span], key_matrix[:, pair_span].T, preferred_element_type=jnp.float32)
            partial_value = partial_value + jnp.dot(value_gradient[:, pair_span], value_matrix[:, pair_span].T, preferred_element_type=jnp.float32)
            summed = summed + rounded(partial_value)
        running_query, running_key, running_value = running
        input_trans = input_seq.T
        running_query = running_query + rounded(jnp.dot(input_trans, grad_query, preferred_element_type=jnp.float32))
        running_key = running_key + rounded(jnp.dot(input_trans, key_gradient, preferred_element_type=jnp.float32))
        running_value = running_value + rounded(jnp.dot(input_trans, value_gradient, preferred_element_type=jnp.float32))
        return ((running_query, running_key, running_value), summed.astype(jnp.bfloat16))
    initial_state = (jnp.zeros((MODEL_FEATURES, QUERY_HEADS * HEAD_SIZE), jnp.float32), jnp.zeros((MODEL_FEATURES, KEY_VALUE_HEADS * HEAD_SIZE), jnp.float32), jnp.zeros((MODEL_FEATURES, KEY_VALUE_HEADS * HEAD_SIZE), jnp.float32))
    sums, input_gradient = lax.scan(one_sequence, initial_state, (inputs, query_states, key_states, saved_value_states, head_cotangent))
    grad_w_query, grad_w_key, grad_w_value = sums
    squared_total = jnp.sum(grad_w_query * grad_w_query) + jnp.sum(grad_w_key * grad_w_key) + jnp.sum(grad_w_value * grad_w_value)
    root_mean_square = jnp.sqrt(squared_total / (MODEL_FEATURES * (QUERY_HEADS + 2 * KEY_VALUE_HEADS) * HEAD_SIZE))
    factor = 1.0 / jnp.maximum(root_mean_square, 1.0)
    query_velocity = 0.9 * query_momentum + factor * grad_w_query
    key_velocity = 0.9 * key_prior_momentum + factor * grad_w_key
    value_velocity = 0.9 * value_prior_momentum + factor * grad_w_value
    return (input_gradient, query_velocity, key_velocity, value_velocity)
```

```python
import functools
import math

import jax
import jax.numpy as jnp
from jax import lax
from jax.experimental import pallas as pl
from jax.experimental.pallas import tpu as pltpu
from jax.sharding import PartitionSpec as P

HEAD_SIZE = 128
MESH = pl.DeviceIdType.MESH
F32 = jnp.float32
BF16 = jnp.bfloat16


def dot(a, b, ca, cb):
    return lax.dot_general(a, b, (((ca,), (cb,)), ((), ())), preferred_element_type=F32)


def kernel(
    nd, total_entries,
    x_ref, q_ref, k_ref, v_ref, do_ref, wq_ref, wk_ref, wv_ref,
    dx_ref, dwq_ref, dwk_ref, dwv_ref, fac_ref,
    g_all, x_all, w_cat, acc, p_buf, y_buf, d_buf, dxr, sqy, sq,
    xs_s, xs_r, xy_s, xy_r, ring_s, ring_r, dd_s, dd_r, py_s, py_r, dx_s, dx_r,
    sqy_s, sqy_r, sq_s, sq_r,
):
    kv = g_all.shape[1]
    seq = g_all.shape[2]
    wide = g_all.shape[3]
    grp = q_ref.shape[2] // k_ref.shape[2]
    gq = grp * HEAD_SIZE
    rows = wq_ref.shape[0]
    half = seq // 2
    nch = nd // 2
    d = lax.axis_index("dp")
    t = lax.axis_index("tensor")
    c = d % 2
    chip = d // 2
    xx = chip % 2
    zz = chip // 2
    pos = zz * (1 - xx) + (nch - 1 - zz) * xx
    dirn = 1 - 2 * c
    partner = chip * 2 + 1 - c

    def chip_of(p):
        p = (p + 2 * nch) % nch
        h = p // (nch // 2)
        z = p * (1 - h) + (nch - 1 - p) * h
        return 2 * z + h

    nxt = chip_of(pos + dirn) * 2 + c

    def ring_src(k):
        return chip_of(pos - dirn * (k + 1)) * 2 + c

    def partner_src(k):
        return chip_of(pos + dirn * (k + 1)) * 2 + 1 - c

    def to(dp, tt):
        return {"dp": dp, "tensor": tt}

    def rcopy(src, dst, ss, rs, dev):
        return pltpu.make_async_remote_copy(
            src_ref=src, dst_ref=dst, send_sem=ss, recv_sem=rs, device_id=dev, device_id_type=MESH
        )

    bar = pltpu.get_barrier_semaphore()

    def sig(i, _):
        pl.semaphore_signal(bar, inc=1, device_id=to((d + i) % nd, t), device_id_type=MESH)
        return 0

    lax.fori_loop(1, nd, sig, 0)
    pl.semaphore_signal(bar, inc=1, device_id=to(d, 1 - t), device_id_type=MESH)

    for j in range(kv):
        w_cat[j, :, 0:gq] = wq_ref[:, j * gq:(j + 1) * gq]
        w_cat[j, :, gq:gq + HEAD_SIZE] = wk_ref[:, j * HEAD_SIZE:(j + 1) * HEAD_SIZE]
        w_cat[j, :, gq + HEAD_SIZE:wide] = wv_ref[:, j * HEAD_SIZE:(j + 1) * HEAD_SIZE]
    acc[...] = jnp.zeros_like(acc)

    pl.semaphore_wait(bar, nd)

    def xcopy(e, slot):
        return rcopy(
            x_ref.at[0, :, pl.ds(pl.multiple_of(e * rows, 128), rows)],
            x_all.at[slot, t], xs_s.at[e], xs_r.at[slot], to(e, t),
        )

    def xsend(i, _):
        xcopy((d + i) % nd, d).start()
        return 0

    lax.fori_loop(1, nd, xsend, 0)
    x_all[d, t] = x_ref[0, :, pl.ds(pl.multiple_of(d * rows, 128), rows)]

    def xfwd(s):
        return rcopy(x_all.at[s, t], x_all.at[s, t], xy_s.at[s], xy_r.at[s], to(d, 1 - t))

    def xfwd_wait(s):
        rcopy(x_all.at[s, 1 - t], x_all.at[s, 1 - t], xy_s.at[s], xy_r.at[s], to(d, 1 - t)).wait_recv()

    xfwd(d).start()

    def ring(step, j, s):
        return rcopy(g_all.at[s, j], g_all.at[s, j], ring_s.at[step, j], ring_r.at[step, j], to(nxt, t))

    def d2d(step, j, s):
        return rcopy(g_all.at[s, j], g_all.at[s, j], dd_s.at[step, j], dd_r.at[step, j], to(partner, t))

    scaling = 1.0 / math.sqrt(HEAD_SIZE)

    def attention(j, _):
        kk = k_ref[0, :, pl.ds(pl.multiple_of(j * HEAD_SIZE, 128), HEAD_SIZE)]
        vv = v_ref[0, :, pl.ds(pl.multiple_of(j * HEAD_SIZE, 128), HEAD_SIZE)]
        dk = jnp.zeros((seq, HEAD_SIZE), F32)
        dv = jnp.zeros((seq, HEAD_SIZE), F32)
        mask = lax.broadcasted_iota(jnp.int32, (seq, seq), 0) >= lax.broadcasted_iota(
            jnp.int32, (seq, seq), 1
        )
        for g in range(grp):
            cols = pl.ds(pl.multiple_of(j * gq + g * HEAD_SIZE, 128), HEAD_SIZE)
            qq = q_ref[0, :, cols]
            oo = do_ref[0, :, cols]
            s = jnp.where(mask, dot(qq, kk, 1, 1) * scaling, -jnp.inf)
            e = jnp.exp(s - jnp.max(s, axis=-1, keepdims=True))
            soft = e / jnp.sum(e, axis=-1, keepdims=True)
            gs = dot(oo, vv, 1, 1)
            delta = jnp.sum(soft * gs, axis=-1, keepdims=True)
            ds = (soft * (gs - delta) * scaling).astype(BF16)
            g_all[d, j, :, g * HEAD_SIZE:(g + 1) * HEAD_SIZE] = dot(ds, kk, 1, 0).astype(BF16)
            dk = dk + dot(ds, qq, 0, 0)
            dv = dv + dot(soft.astype(BF16), oo, 0, 0)
        g_all[d, j, :, gq:gq + HEAD_SIZE] = dk.astype(BF16)
        g_all[d, j, :, gq + HEAD_SIZE:wide] = dv.astype(BF16)
        ring(0, j, d).start()
        d2d(0, j, d).start()
        return 0

    lax.fori_loop(0, kv, attention, 0)

    def xready(s):
        xcopy(s, s).wait_recv()
        xfwd(s).start()

    def pcopy(s):
        return rcopy(p_buf.at[s, 1 - t], y_buf.at[s], py_s.at[s], py_r.at[s], to(d, 1 - t))

    def block(s):
        xfwd_wait(s)
        xb = x_all[s].reshape(seq, rows)
        part = jnp.zeros((seq, rows), F32)
        for j in range(kv):
            gb = g_all[s, j]
            part = part + dot(gb, w_cat[j], 1, 1)
            acc[j] += dot(xb, gb, 0, 0)
        p_buf[s] = part.astype(BF16).reshape(2, half, rows)
        pcopy(s).start()

    def reduced(s):
        pcopy(s).wait_recv()
        return (p_buf[s, t].astype(F32) + y_buf[s].astype(F32)).astype(BF16)

    def dxcopy(s, slot):
        return rcopy(d_buf.at[s], dxr.at[slot], dx_s.at[s], dx_r.at[slot], to(s, t))

    def finish(s):
        d_buf[s] = reduced(s)
        dxcopy(s, d).start()

    xready(partner)
    block(d)
    for j in range(kv):
        d2d(0, j, partner).wait_recv()
    block(partner)
    dxr[d] = reduced(d)
    steps = nch - 1

    def step(k, _):
        sa = ring_src(k)
        sb = partner_src(k)
        xready(sa)
        xready(sb)
        for j in range(kv):
            ring(k, j, sa).wait_recv()

            @pl.when(k < steps - 1)
            def _():
                ring(k + 1, j, sa).start()

            d2d(k + 1, j, sa).start()
        block(sa)
        for j in range(kv):
            d2d(k + 1, j, sb).wait_recv()
        block(sb)

        @pl.when(k == 0)
        def _():
            finish(partner)

        @pl.when(k > 0)
        def _():
            finish(ring_src(k - 1))
            finish(partner_src(k - 1))

        return 0

    lax.fori_loop(0, steps, step, 0)

    squares = jnp.zeros((1, 1), F32)
    for j in range(kv):
        a = acc[j]
        squares = squares + jnp.sum(a * a, keepdims=True)
    sqy[t] = jnp.broadcast_to(squares, (8, 128))
    sqc = rcopy(sqy.at[t], sqy.at[t], sqy_s, sqy_r, to(d, 1 - t))
    sqc.start()
    finish(ring_src(steps - 1))
    finish(partner_src(steps - 1))
    rcopy(sqy.at[1 - t], sqy.at[1 - t], sqy_s, sqy_r, to(d, 1 - t)).wait_recv()
    sq[d] = sqy[0] + sqy[1]

    def sqcopy(e, slot):
        return rcopy(sq.at[slot], sq.at[slot], sq_s.at[e], sq_r.at[slot], to(e, t))

    def sqsend(i, _):
        sqcopy((d + i) % nd, d).start()
        return 0

    lax.fori_loop(1, nd, sqsend, 0)
    for j in range(kv):
        dwq_ref[:, j * gq:(j + 1) * gq] = acc[j, :, 0:gq]
        dwk_ref[:, j * HEAD_SIZE:(j + 1) * HEAD_SIZE] = acc[j, :, gq:gq + HEAD_SIZE]
        dwv_ref[:, j * HEAD_SIZE:(j + 1) * HEAD_SIZE] = acc[j, :, gq + HEAD_SIZE:wide]

    def drain(i, _):
        e = (d + i) % nd
        xcopy(e, d).wait_send()
        dxcopy(e, d).wait_send()
        dxcopy(e, e).wait_recv()
        sqcopy(e, d).wait_send()
        sqcopy(e, e).wait_recv()
        return 0

    lax.fori_loop(1, nd, drain, 0)

    def drain_all(s, _):
        xfwd(s).wait_send()
        pcopy(s).wait_send()
        return 0

    lax.fori_loop(0, nd, drain_all, 0)
    sqc.wait_send()
    for j in range(kv):
        def drain_g(k, _):
            ring(k, j, d).wait_send()
            d2d(k, j, d).wait_send()
            return 0

        lax.fori_loop(0, steps, drain_g, 0)
        d2d(steps, j, d).wait_send()
    for e in range(nd):
        dx_ref[0, :, e * rows:(e + 1) * rows] = dxr[e]
    total = jnp.sum(sq[...], axis=0)
    fac_ref[...] = 1.0 / jnp.maximum(jnp.sqrt(total / total_entries), 1.0)


def fused(nd, nt, inputs, q, k, v, do, wq, wk, wv):
    seq = q.shape[1]
    kv = k.shape[2] // HEAD_SIZE
    wide = (q.shape[2] + 2 * k.shape[2]) // kv
    rows = wq.shape[0]
    half = seq // nt
    total_entries = float(rows * nd * kv * wide * nt)
    vm = pl.BlockSpec(memory_space=pltpu.VMEM)
    dma = pltpu.SemaphoreType.DMA
    steps = nd // 2 - 1
    return pl.pallas_call(
        functools.partial(kernel, nd, total_entries),
        out_shape=(
            jax.ShapeDtypeStruct(inputs.shape, BF16),
            jax.ShapeDtypeStruct(wq.shape, F32),
            jax.ShapeDtypeStruct(wk.shape, F32),
            jax.ShapeDtypeStruct(wv.shape, F32),
            jax.ShapeDtypeStruct((8, 128), F32),
        ),
        in_specs=[vm] * 8,
        out_specs=(vm,) * 5,
        scratch_shapes=[
            pltpu.VMEM((nd, kv, seq, wide), BF16),
            pltpu.VMEM((nd, nt, half, rows), BF16),
            pltpu.VMEM((kv, rows, wide), BF16),
            pltpu.VMEM((kv, rows, wide), F32),
            pltpu.VMEM((nd, nt, half, rows), BF16),
            pltpu.VMEM((nd, half, rows), BF16),
            pltpu.VMEM((nd, half, rows), BF16),
            pltpu.VMEM((nd, half, rows), BF16),
            pltpu.VMEM((2, 8, 128), F32),
            pltpu.VMEM((nd, 8, 128), F32),
            dma((nd,)), dma((nd,)), dma((nd,)), dma((nd,)),
            dma((steps, kv)), dma((steps, kv)), dma((steps + 1, kv)), dma((steps + 1, kv)),
            dma((nd,)), dma((nd,)), dma((nd,)), dma((nd,)),
            dma, dma, dma((nd,)), dma((nd,)),
        ],
        compiler_params=pltpu.CompilerParams(
            collective_id=0, has_side_effects=True, vmem_limit_bytes=60 * 1024 * 1024
        ),
    )(inputs, q, k, v, do, wq, wk, wv)


def heads_backward(query_row_set, key_rows, value_rows, cotangent_rows):
    token_length = query_row_set.shape[0]
    kv_heads = key_rows.shape[1] // HEAD_SIZE
    group_width = query_row_set.shape[1] // HEAD_SIZE // kv_heads
    scaling = 1.0 / math.sqrt(HEAD_SIZE)
    query_quad = query_row_set.reshape(token_length, kv_heads, group_width, HEAD_SIZE)
    cotangent_quad = cotangent_rows.reshape(token_length, kv_heads, group_width, HEAD_SIZE)
    key_triple = key_rows.reshape(token_length, kv_heads, HEAD_SIZE)
    value_triple = value_rows.reshape(token_length, kv_heads, HEAD_SIZE)
    block_rows = min(token_length, 512)
    key_sums = jnp.zeros((token_length, kv_heads, HEAD_SIZE), F32)
    value_sums = jnp.zeros((token_length, kv_heads, HEAD_SIZE), F32)
    query_blocks = []
    for row_start in range(0, token_length, block_rows):
        row_end = row_start + block_rows
        query_block = query_quad[row_start:row_end]
        cotangent_block = cotangent_quad[row_start:row_end]
        key_block = key_triple[:row_end]
        value_block = value_triple[:row_end]
        scores = (
            jnp.einsum("ihgd,jhd->hgij", query_block, key_block, preferred_element_type=F32)
            * scaling
        )
        query_index = row_start + lax.broadcasted_iota(jnp.int32, (block_rows, row_end), 0)
        key_index = lax.broadcasted_iota(jnp.int32, (block_rows, row_end), 1)
        scores = jnp.where(query_index >= key_index, scores, -jnp.inf)
        maximum = jnp.max(scores, axis=-1, keepdims=True)
        exponent = jnp.exp(scores - maximum)
        softmax_rows = exponent / jnp.sum(exponent, axis=-1, keepdims=True)
        softmax_reduced = softmax_rows.astype(BF16)
        grad_softmax = jnp.einsum(
            "ihgd,jhd->hgij", cotangent_block, value_block, preferred_element_type=F32
        )
        row_delta = jnp.sum(softmax_rows * grad_softmax, axis=-1, keepdims=True)
        score_gradient = (softmax_rows * (grad_softmax - row_delta) * scaling).astype(BF16)
        query_blocks.append(
            jnp.einsum(
                "hgij,jhd->ihgd", score_gradient, key_block, preferred_element_type=F32
            ).astype(BF16)
        )
        key_sums = key_sums.at[:row_end].add(
            jnp.einsum(
                "xfwo,wxfp->oxp", score_gradient, query_block, preferred_element_type=F32
            )
        )
        value_sums = value_sums.at[:row_end].add(
            jnp.einsum(
                "xfwo,wxfp->oxp",
                softmax_reduced,
                cotangent_block,
                preferred_element_type=F32,
            )
        )
    grad_query = jnp.concatenate(query_blocks, axis=0).reshape(token_length, -1)
    key_gradient = key_sums.astype(BF16).reshape(token_length, -1)
    value_gradient = value_sums.astype(BF16).reshape(token_length, -1)
    return (grad_query, key_gradient, value_gradient)


def small(nd, nt, inputs, query_states, key_states, query_weight):
    seq = query_states.shape[1]
    cols = query_states.shape[2] + 2 * key_states.shape[2]
    held = nd * seq * cols * 2 + 10 * nd * seq * query_weight.shape[0]
    return nt == 2 and nd % 4 == 0 and nd >= 8 and held < 36 * 1024 * 1024


def local(nd, nt, *args):
    inputs, q, k, v, do, wq, wk, wv, mq, mk, mv = args
    if small(nd, nt, inputs, q, k, wq):
        grad_inputs, gq, gk, gv, fac = fused(nd, nt, inputs, q, k, v, do, wq, wk, wv)
        factor = fac[0, 0]
    else:
        query_cols = wq.shape[1]
        pair_cols = wk.shape[1]
        rows = wq.shape[0]
        weights = jnp.concatenate((wq, wk, wv), axis=1)
        grads = jnp.concatenate(heads_backward(q[0], k[0], v[0], do[0]), axis=1)
        all_grads = lax.all_gather(grads, "dp", axis=0, tiled=True)
        pieces = lax.all_to_all(inputs[0], "dp", 1, 0, tiled=True)
        pieces = pieces.reshape(nd, -1, rows)
        all_inputs = lax.all_gather(pieces, "tensor", axis=1, tiled=True).reshape(-1, rows)
        summed = dot(all_inputs, all_grads, 0, 0)
        parts = dot(all_grads, weights, 1, 1).astype(BF16).reshape(nd, -1, rows)
        mine = lax.psum_scatter(parts, "tensor", scatter_dimension=1, tiled=True)
        grad_inputs = lax.all_to_all(mine.reshape(-1, rows), "dp", 0, 1, tiled=True)[None]
        total = lax.psum(jnp.sum(summed * summed), ("dp", "tensor"))
        factor = 1.0 / jnp.maximum(jnp.sqrt(total / (summed.size * nd * nt)), 1.0)
        gq = summed[:, :query_cols]
        gk = summed[:, query_cols:query_cols + pair_cols]
        gv = summed[:, query_cols + pair_cols:]
    return (
        grad_inputs,
        0.9 * mq + factor * gq,
        0.9 * mk + factor * gk,
        0.9 * mv + factor * gv,
    )


def solution(mesh):
    nd, nt = mesh.shape["dp"], mesh.shape["tensor"]
    saved = P("dp", None, "tensor")
    tokens = P("dp", "tensor", None)
    weight = P("dp", "tensor")
    return jax.shard_map(
        functools.partial(local, nd, nt),
        mesh=mesh,
        in_specs=(tokens,) + (saved,) * 4 + (weight,) * 6,
        out_specs=(tokens,) + (weight,) * 3,
        check_vma=False,
    )
```

```python
import functools
import math

import jax
import jax.numpy as jnp
from jax import lax
from jax.experimental import pallas as pl
from jax.experimental.pallas import tpu as pltpu
from jax.sharding import PartitionSpec as P

HEAD_SIZE = 128
MESH = pl.DeviceIdType.MESH
F32 = jnp.float32
BF16 = jnp.bfloat16


def dot(a, b, ca, cb):
    return lax.dot_general(a, b, (((ca,), (cb,)), ((), ())), preferred_element_type=F32)


def kernel(
    nd, total_entries,
    x_ref, q_ref, k_ref, v_ref, do_ref, wq_ref, wk_ref, wv_ref,
    dx_ref, dwq_ref, dwk_ref, dwv_ref, fac_ref,
    g_all, x_all, w_cat, acc, p_buf, y_buf, d_buf, dxr, sqy, sq, xt, part,
    xs_s, xs_r, xy_s, xy_r, ring_s, ring_r, dd_s, dd_r, py_s, py_r, dx_s, dx_r,
    sqy_s, sqy_r, sq_s, sq_r,
):
    kv = g_all.shape[1]
    seq = g_all.shape[2]
    wide = g_all.shape[3]
    grp = q_ref.shape[2] // k_ref.shape[2]
    gq = grp * HEAD_SIZE
    rows = wq_ref.shape[0]
    half = seq // 2
    nch = nd // 2
    d = lax.axis_index("dp")
    t = lax.axis_index("tensor")
    c = d % 2
    chip = d // 2
    xx = chip % 2
    zz = chip // 2
    pos = zz * (1 - xx) + (nch - 1 - zz) * xx
    dirn = 1 - 2 * c
    partner = chip * 2 + 1 - c

    def chip_of(p):
        p = (p + 2 * nch) % nch
        h = p // (nch // 2)
        z = p * (1 - h) + (nch - 1 - p) * h
        return 2 * z + h

    nxt = chip_of(pos + dirn) * 2 + c

    def ring_src(k):
        return chip_of(pos - dirn * (k + 1)) * 2 + c

    def partner_src(k):
        return chip_of(pos + dirn * (k + 1)) * 2 + 1 - c

    def to(dp, tt):
        return {"dp": dp, "tensor": tt}

    def rcopy(src, dst, ss, rs, dev):
        return pltpu.make_async_remote_copy(
            src_ref=src, dst_ref=dst, send_sem=ss, recv_sem=rs, device_id=dev, device_id_type=MESH
        )

    bar = pltpu.get_barrier_semaphore()

    def sig(i, _):
        pl.semaphore_signal(bar, inc=1, device_id=to((d + i) % nd, t), device_id_type=MESH)
        return 0

    lax.fori_loop(1, nd, sig, 0)
    pl.semaphore_signal(bar, inc=1, device_id=to(d, 1 - t), device_id_type=MESH)

    for j in range(kv):
        w_cat[j, :, 0:gq] = wq_ref[:, j * gq:(j + 1) * gq]
        w_cat[j, :, gq:gq + HEAD_SIZE] = wk_ref[:, j * HEAD_SIZE:(j + 1) * HEAD_SIZE]
        w_cat[j, :, gq + HEAD_SIZE:wide] = wv_ref[:, j * HEAD_SIZE:(j + 1) * HEAD_SIZE]
    acc[...] = jnp.zeros_like(acc)

    pl.semaphore_wait(bar, nd)

    def xcopy(e, slot):
        return rcopy(
            x_ref.at[0, :, pl.ds(pl.multiple_of(e * rows, 128), rows)],
            x_all.at[slot, t], xs_s.at[e], xs_r.at[slot], to(e, t),
        )

    def xsend(i, _):
        xcopy((d + i) % nd, d).start()
        return 0

    lax.fori_loop(1, nd, xsend, 0)
    x_all[d, t] = x_ref[0, :, pl.ds(pl.multiple_of(d * rows, 128), rows)]

    def xfwd(s):
        return rcopy(x_all.at[s, t], x_all.at[s, t], xy_s.at[s], xy_r.at[s], to(d, 1 - t))

    def xfwd_wait(s):
        rcopy(x_all.at[s, 1 - t], x_all.at[s, 1 - t], xy_s.at[s], xy_r.at[s], to(d, 1 - t)).wait_recv()

    xfwd(d).start()

    def ring(step, j, s):
        return rcopy(g_all.at[s, j], g_all.at[s, j], ring_s.at[step, j], ring_r.at[step, j], to(nxt, t))

    def d2d(step, j, s):
        return rcopy(g_all.at[s, j], g_all.at[s, j], dd_s.at[step, j], dd_r.at[step, j], to(partner, t))

    scaling = 1.0 / math.sqrt(HEAD_SIZE)

    def attention(j, _):
        kk = k_ref[0, :, pl.ds(pl.multiple_of(j * HEAD_SIZE, 128), HEAD_SIZE)]
        vv = v_ref[0, :, pl.ds(pl.multiple_of(j * HEAD_SIZE, 128), HEAD_SIZE)]
        dk = jnp.zeros((seq, HEAD_SIZE), F32)
        dv = jnp.zeros((seq, HEAD_SIZE), F32)
        mask = lax.broadcasted_iota(jnp.int32, (seq, seq), 0) >= lax.broadcasted_iota(
            jnp.int32, (seq, seq), 1
        )
        for g in range(grp):
            cols = pl.ds(pl.multiple_of(j * gq + g * HEAD_SIZE, 128), HEAD_SIZE)
            qq = q_ref[0, :, cols]
            oo = do_ref[0, :, cols]
            s = jnp.where(mask, dot(qq, kk, 1, 1) * scaling, -jnp.inf)
            e = jnp.exp(s - jnp.max(s, axis=-1, keepdims=True))
            soft = e / jnp.sum(e, axis=-1, keepdims=True)
            gs = dot(oo, vv, 1, 1)
            delta = jnp.sum(soft * gs, axis=-1, keepdims=True)
            ds = (soft * (gs - delta) * scaling).astype(BF16)
            g_all[d, j, :, g * HEAD_SIZE:(g + 1) * HEAD_SIZE] = dot(ds, kk, 1, 0).astype(BF16)
            dk = dk + dot(ds, qq, 0, 0)
            dv = dv + dot(soft.astype(BF16), oo, 0, 0)
        g_all[d, j, :, gq:gq + HEAD_SIZE] = dk.astype(BF16)
        g_all[d, j, :, gq + HEAD_SIZE:wide] = dv.astype(BF16)
        ring(0, j, d).start()
        d2d(0, j, d).start()
        return 0

    lax.fori_loop(0, kv, attention, 0)

    def xready(s):
        xcopy(s, s).wait_recv()
        xfwd(s).start()

    def pcopy(s):
        return rcopy(p_buf.at[s, 1 - t], y_buf.at[s], py_s.at[s], py_r.at[s], to(d, 1 - t))

    def load_x(a, b):
        for n, s in enumerate((a, b)):
            xfwd_wait(s)
            xt[n] = x_all[s].reshape(seq, rows).T

    def chunk(j, a, b):
        ga = g_all[a, j]
        gb = g_all[b, j]
        acc[j] += dot(xt[0], ga, 1, 0) + dot(xt[1], gb, 1, 0)
        pa = dot(ga, w_cat[j], 1, 1)
        pb = dot(gb, w_cat[j], 1, 1)
        part[0] = pa if j == 0 else part[0] + pa
        part[1] = pb if j == 0 else part[1] + pb

    def send_parts(a, b):
        for n, s in enumerate((a, b)):
            p_buf[s] = part[n].astype(BF16).reshape(2, half, rows)
            pcopy(s).start()

    def reduced(s):
        pcopy(s).wait_recv()
        return (p_buf[s, t].astype(F32) + y_buf[s].astype(F32)).astype(BF16)

    def dxcopy(s, slot):
        return rcopy(d_buf.at[s], dxr.at[slot], dx_s.at[s], dx_r.at[slot], to(s, t))

    def finish(s):
        d_buf[s] = reduced(s)
        dxcopy(s, d).start()

    steps = nch - 1

    def arrive(k, j, sa):
        ring(k, j, sa).wait_recv()

        @pl.when(k < steps - 1)
        def _():
            ring(k + 1, j, sa).start()

        d2d(k + 1, j, sa).start()

    xready(partner)
    sa = ring_src(0)
    sb = partner_src(0)
    xready(sa)
    xready(sb)
    load_x(d, partner)
    for j in range(kv):
        arrive(0, j, sa)
        d2d(0, j, partner).wait_recv()
        chunk(j, d, partner)
    send_parts(d, partner)
    load_x(sa, sb)
    for j in range(kv):
        d2d(1, j, sb).wait_recv()
        chunk(j, sa, sb)
    send_parts(sa, sb)
    dxr[d] = reduced(d)
    finish(partner)

    def step(k, _):
        sa = ring_src(k)
        sb = partner_src(k)
        xready(sa)
        xready(sb)
        for j in range(kv):
            arrive(k, j, sa)
            if j == 0:
                load_x(sa, sb)
            d2d(k + 1, j, sb).wait_recv()
            chunk(j, sa, sb)
            if j == 0:
                finish(ring_src(k - 1))
                finish(partner_src(k - 1))
        send_parts(sa, sb)
        return 0

    lax.fori_loop(1, steps, step, 0)

    squares = jnp.zeros((1, 1), F32)
    for j in range(kv):
        a = acc[j]
        squares = squares + jnp.sum(a * a, keepdims=True)
    sqy[t] = jnp.broadcast_to(squares, (8, 128))
    sqc = rcopy(sqy.at[t], sqy.at[t], sqy_s, sqy_r, to(d, 1 - t))
    sqc.start()
    finish(ring_src(steps - 1))
    finish(partner_src(steps - 1))
    rcopy(sqy.at[1 - t], sqy.at[1 - t], sqy_s, sqy_r, to(d, 1 - t)).wait_recv()
    sq[d] = sqy[0] + sqy[1]

    def sqcopy(e, slot):
        return rcopy(sq.at[slot], sq.at[slot], sq_s.at[e], sq_r.at[slot], to(e, t))

    def sqsend(i, _):
        sqcopy((d + i) % nd, d).start()
        return 0

    lax.fori_loop(1, nd, sqsend, 0)
    for j in range(kv):
        dwq_ref[:, j * gq:(j + 1) * gq] = acc[j, :, 0:gq]
        dwk_ref[:, j * HEAD_SIZE:(j + 1) * HEAD_SIZE] = acc[j, :, gq:gq + HEAD_SIZE]
        dwv_ref[:, j * HEAD_SIZE:(j + 1) * HEAD_SIZE] = acc[j, :, gq + HEAD_SIZE:wide]

    def drain(i, _):
        e = (d + i) % nd
        xcopy(e, d).wait_send()
        dxcopy(e, d).wait_send()
        dxcopy(e, e).wait_recv()
        sqcopy(e, d).wait_send()
        sqcopy(e, e).wait_recv()
        return 0

    lax.fori_loop(1, nd, drain, 0)

    def drain_all(s, _):
        xfwd(s).wait_send()
        pcopy(s).wait_send()
        return 0

    lax.fori_loop(0, nd, drain_all, 0)
    sqc.wait_send()
    for j in range(kv):
        def drain_g(k, _):
            ring(k, j, d).wait_send()
            d2d(k, j, d).wait_send()
            return 0

        lax.fori_loop(0, steps, drain_g, 0)
        d2d(steps, j, d).wait_send()
    for e in range(nd):
        dx_ref[0, :, e * rows:(e + 1) * rows] = dxr[e]
    total = jnp.sum(sq[...], axis=0)
    fac_ref[...] = 1.0 / jnp.maximum(jnp.sqrt(total / total_entries), 1.0)


def fused(nd, nt, inputs, q, k, v, do, wq, wk, wv):
    seq = q.shape[1]
    kv = k.shape[2] // HEAD_SIZE
    wide = (q.shape[2] + 2 * k.shape[2]) // kv
    rows = wq.shape[0]
    half = seq // nt
    total_entries = float(rows * nd * kv * wide * nt)
    vm = pl.BlockSpec(memory_space=pltpu.VMEM)
    dma = pltpu.SemaphoreType.DMA
    steps = nd // 2 - 1
    return pl.pallas_call(
        functools.partial(kernel, nd, total_entries),
        out_shape=(
            jax.ShapeDtypeStruct(inputs.shape, BF16),
            jax.ShapeDtypeStruct(wq.shape, F32),
            jax.ShapeDtypeStruct(wk.shape, F32),
            jax.ShapeDtypeStruct(wv.shape, F32),
            jax.ShapeDtypeStruct((8, 128), F32),
        ),
        in_specs=[vm] * 8,
        out_specs=(vm,) * 5,
        scratch_shapes=[
            pltpu.VMEM((nd, kv, seq, wide), BF16),
            pltpu.VMEM((nd, nt, half, rows), BF16),
            pltpu.VMEM((kv, rows, wide), BF16),
            pltpu.VMEM((kv, rows, wide), F32),
            pltpu.VMEM((nd, nt, half, rows), BF16),
            pltpu.VMEM((nd, half, rows), BF16),
            pltpu.VMEM((nd, half, rows), BF16),
            pltpu.VMEM((nd, half, rows), BF16),
            pltpu.VMEM((2, 8, 128), F32),
            pltpu.VMEM((nd, 8, 128), F32),
            pltpu.VMEM((2, rows, seq), BF16),
            pltpu.VMEM((2, seq, rows), F32),
            dma((nd,)), dma((nd,)), dma((nd,)), dma((nd,)),
            dma((steps, kv)), dma((steps, kv)), dma((steps + 1, kv)), dma((steps + 1, kv)),
            dma((nd,)), dma((nd,)), dma((nd,)), dma((nd,)),
            dma, dma, dma((nd,)), dma((nd,)),
        ],
        compiler_params=pltpu.CompilerParams(
            collective_id=0, has_side_effects=True, vmem_limit_bytes=60 * 1024 * 1024
        ),
    )(inputs, q, k, v, do, wq, wk, wv)


def heads_backward(query_row_set, key_rows, value_rows, cotangent_rows):
    token_length = query_row_set.shape[0]
    kv_heads = key_rows.shape[1] // HEAD_SIZE
    group_width = query_row_set.shape[1] // HEAD_SIZE // kv_heads
    scaling = 1.0 / math.sqrt(HEAD_SIZE)
    query_quad = query_row_set.reshape(token_length, kv_heads, group_width, HEAD_SIZE)
    cotangent_quad = cotangent_rows.reshape(token_length, kv_heads, group_width, HEAD_SIZE)
    key_triple = key_rows.reshape(token_length, kv_heads, HEAD_SIZE)
    value_triple = value_rows.reshape(token_length, kv_heads, HEAD_SIZE)
    block_rows = min(token_length, 512)
    key_sums = jnp.zeros((token_length, kv_heads, HEAD_SIZE), F32)
    value_sums = jnp.zeros((token_length, kv_heads, HEAD_SIZE), F32)
    query_blocks = []
    for row_start in range(0, token_length, block_rows):
        row_end = row_start + block_rows
        query_block = query_quad[row_start:row_end]
        cotangent_block = cotangent_quad[row_start:row_end]
        key_block = key_triple[:row_end]
        value_block = value_triple[:row_end]
        scores = (
            jnp.einsum("ihgd,jhd->hgij", query_block, key_block, preferred_element_type=F32)
            * scaling
        )
        query_index = row_start + lax.broadcasted_iota(jnp.int32, (block_rows, row_end), 0)
        key_index = lax.broadcasted_iota(jnp.int32, (block_rows, row_end), 1)
        scores = jnp.where(query_index >= key_index, scores, -jnp.inf)
        maximum = jnp.max(scores, axis=-1, keepdims=True)
        exponent = jnp.exp(scores - maximum)
        softmax_rows = exponent / jnp.sum(exponent, axis=-1, keepdims=True)
        softmax_reduced = softmax_rows.astype(BF16)
        grad_softmax = jnp.einsum(
            "ihgd,jhd->hgij", cotangent_block, value_block, preferred_element_type=F32
        )
        row_delta = jnp.sum(softmax_rows * grad_softmax, axis=-1, keepdims=True)
        score_gradient = (softmax_rows * (grad_softmax - row_delta) * scaling).astype(BF16)
        query_blocks.append(
            jnp.einsum(
                "hgij,jhd->ihgd", score_gradient, key_block, preferred_element_type=F32
            ).astype(BF16)
        )
        key_sums = key_sums.at[:row_end].add(
            jnp.einsum(
                "xfwo,wxfp->oxp", score_gradient, query_block, preferred_element_type=F32
            )
        )
        value_sums = value_sums.at[:row_end].add(
            jnp.einsum(
                "xfwo,wxfp->oxp",
                softmax_reduced,
                cotangent_block,
                preferred_element_type=F32,
            )
        )
    grad_query = jnp.concatenate(query_blocks, axis=0).reshape(token_length, -1)
    key_gradient = key_sums.astype(BF16).reshape(token_length, -1)
    value_gradient = value_sums.astype(BF16).reshape(token_length, -1)
    return (grad_query, key_gradient, value_gradient)


def small(nd, nt, inputs, query_states, key_states, query_weight):
    seq = query_states.shape[1]
    cols = query_states.shape[2] + 2 * key_states.shape[2]
    held = nd * seq * cols * 2 + 10 * nd * seq * query_weight.shape[0]
    return nt == 2 and nd % 4 == 0 and nd >= 8 and held < 36 * 1024 * 1024


def local(nd, nt, *args):
    inputs, q, k, v, do, wq, wk, wv, mq, mk, mv = args
    if small(nd, nt, inputs, q, k, wq):
        grad_inputs, gq, gk, gv, fac = fused(nd, nt, inputs, q, k, v, do, wq, wk, wv)
        factor = fac[0, 0]
    else:
        query_cols = wq.shape[1]
        pair_cols = wk.shape[1]
        rows = wq.shape[0]
        weights = jnp.concatenate((wq, wk, wv), axis=1)
        grads = jnp.concatenate(heads_backward(q[0], k[0], v[0], do[0]), axis=1)
        all_grads = lax.all_gather(grads, "dp", axis=0, tiled=True)
        pieces = lax.all_to_all(inputs[0], "dp", 1, 0, tiled=True)
        pieces = pieces.reshape(nd, -1, rows)
        all_inputs = lax.all_gather(pieces, "tensor", axis=1, tiled=True).reshape(-1, rows)
        summed = dot(all_inputs, all_grads, 0, 0)
        parts = dot(all_grads, weights, 1, 1).astype(BF16).reshape(nd, -1, rows)
        mine = lax.psum_scatter(parts, "tensor", scatter_dimension=1, tiled=True)
        grad_inputs = lax.all_to_all(mine.reshape(-1, rows), "dp", 0, 1, tiled=True)[None]
        total = lax.psum(jnp.sum(summed * summed), ("dp", "tensor"))
        factor = 1.0 / jnp.maximum(jnp.sqrt(total / (summed.size * nd * nt)), 1.0)
        gq = summed[:, :query_cols]
        gk = summed[:, query_cols:query_cols + pair_cols]
        gv = summed[:, query_cols + pair_cols:]
    return (
        grad_inputs,
        0.9 * mq + factor * gq,
        0.9 * mk + factor * gk,
        0.9 * mv + factor * gv,
    )


def solution(mesh):
    nd, nt = mesh.shape["dp"], mesh.shape["tensor"]
    saved = P("dp", None, "tensor")
    tokens = P("dp", "tensor", None)
    weight = P("dp", "tensor")
    return jax.shard_map(
        functools.partial(local, nd, nt),
        mesh=mesh,
        in_specs=(tokens,) + (saved,) * 4 + (weight,) * 6,
        out_specs=(tokens,) + (weight,) * 3,
        check_vma=False,
    )
```
